32 devices in a mesh: gx: 4 (over x, core), gy: 2 (over y), gz: 4 (over z).
Axes of the slice: x: 2, y: 2, z: 4, core: 2. Of those that a mesh axis runs over, the one named last changes fastest.
Arguments:
- opening_warmth_field: float32 [32, 32, 512], P('gx', 'gy', 'gz'), may hold values from -42 to 42
- cellwise_warming_source: float32 [32, 32, 512], P('gx', 'gy', 'gz'), may hold values from -6 to 6
- substance_category_per_voxel: int32 [32, 32, 512], P('gx', 'gy', 'gz'), may hold values from 0 to 15
- thermal_coefficient_table: float32 [16], replicated, may hold values from 0.2 to 5
- boundary_cooling_flags: int32 [32, 32, 512], P('gx', 'gy', 'gz'), may hold values 0 or 1
Outputs:
- closing_warmth_field: float32 [32, 32, 512], P('gx', 'gy', 'gz')
- remaining_mismatch: float32 [32, 32, 512], P('gx', 'gy', 'gz')
The draws below stay inside these ranges and needn't reach their ends.
All inputs are finite; a program needn't handle non-finite values. No bound on the sum of `boundary_cooling_flags` on one device may be relied on, other than what follows from the above.
Results may differ from the reference program's by a relative error of at most 0.00055.
Values sent between devices are 32-bit elements; how exact they have to be, the bound alone decides.
A program may use at most 64 MiB of HBM per device.

```python
import math
import jax
import jax.numpy as jnp
from jax import lax

ITERS = 4
TSTEPS = 1
CLASSES = 16
NX = 32
NY = 32
NZ = 512


def draw_opening_warmth_field(key, part):
    keys = jax.random.split(key, 1)
    ramp = (1.0 + 2.0 * jnp.arange(NX, dtype=jnp.float32) / (NX - 1))[:, None, None]
    values = jax.random.truncated_normal(keys[0], -5.0, 5.0, (NX, NY, NZ), jnp.float32) * ramp
    return values.astype(jnp.float32)


def place_ends(entries, key, least, top_value):
    longest = entries.shape.index(max(entries.shape))
    spots = []
    for shift in (0, 1):
        where = [jax.random.randint(jax.random.fold_in(key, axis), (), 0, length) for axis, length in enumerate(entries.shape)]
        where[longest] = (where[longest] + shift) % entries.shape[longest]
        spots.append(tuple(where))
    return entries.at[spots[0]].set(least).at[spots[1]].set(top_value)


def block_scale(stream_key, extent, cuts, least, high):
    def one(dim, blocks):
        draws = jax.random.uniform(jax.random.fold_in(jax.random.fold_in(stream_key, 6), dim), (blocks,), jnp.float32, least / len(cuts), high / len(cuts))
        return jnp.repeat(jnp.exp(draws), extent[dim] // blocks).reshape((-1,) + (1,) * (len(extent) - dim - 1))

    factor_of = one(*cuts[0])
    for cut in cuts[1:]:
        factor_of = factor_of * one(*cut)
    return factor_of


def normal_values(own_key, shape, scale, reach, cuts=(), held_as=jnp.bfloat16):
    loudness = block_scale(own_key, shape, cuts, -0.22, 0.18) if cuts else 1.0
    drawn = jax.random.normal(own_key, shape, jnp.float32) * scale * loudness
    return jnp.minimum(jnp.maximum(drawn, -reach), reach).astype(held_as)


def setup_inputs(seed: int = 0) -> dict:
    key_list = jax.random.split(jax.random.key(seed), 6)
    opening_warmth_field = draw_opening_warmth_field(jax.random.fold_in(key_list[5], 71), 0)
    cellwise_warming_source = normal_values(key_list[1], (NX, NY, NZ), 1.0, 6.0, ((0, 4), (1, 2), (2, 4)), jnp.float32)
    substance_category_per_voxel = place_ends(jax.random.randint(key_list[2], (NX, NY, NZ), 0, CLASSES), jax.random.fold_in(key_list[2], 1), 0, CLASSES - 1).astype(jnp.int32)
    thermal_coefficient_table = jnp.clip(jnp.exp(jax.random.uniform(key_list[3], (CLASSES,), jnp.float32, math.log(0.2), math.log(5.0))), 0.2, 5.0)
    boundary_cooling_flags = place_ends((jax.random.randint(key_list[4], (NX, NY, NZ), 0, 4) < 1).astype(jnp.int32), jax.random.fold_in(key_list[4], 1), 0, 1)
    return {"opening_warmth_field": opening_warmth_field, "cellwise_warming_source": cellwise_warming_source, "substance_category_per_voxel": substance_category_per_voxel, "thermal_coefficient_table": thermal_coefficient_table, "boundary_cooling_flags": boundary_cooling_flags}


interval_delta = 2.0
cooling = 3.0
kind_weights = (1.0, 0.5, 0.25)
kind_counts = (6.0, 12.0, 8.0)


def split_axis(values, axis):
    length = values.shape[axis] - 2
    center = lax.slice_in_dim(values, 1, length + 1, axis=axis)
    beside = lax.slice_in_dim(values, 0, length, axis=axis) + lax.slice_in_dim(values, 2, length + 2, axis=axis)
    return center, beside


def neighbor_sums(padded):
    leading_extent = padded.ndim - 3
    pieces = [(padded, 0)]
    for shift_vector in range(3):
        next_pieces = []
        for values, neighbors in pieces:
            center, beside = split_axis(values, leading_extent + shift_vector)
            next_pieces.append((center, neighbors))
            next_pieces.append((beside, neighbors + 1))
        pieces = next_pieces
    totals = [None, None, None]
    for values, neighbors in pieces:
        if neighbors > 0:
            if totals[neighbors - 1] is None:
                totals[neighbors - 1] = values
            else:
                totals[neighbors - 1] = totals[neighbors - 1] + values
    return totals


def coupling(padded, padded_flux, cond):
    field_sums = neighbor_sums(padded)
    accumulated_flux = neighbor_sums(padded_flux)
    computed_output = kind_weights[0] * (cond * field_sums[0] + accumulated_flux[0])
    computed_output = computed_output + kind_weights[1] * (cond * field_sums[1] + accumulated_flux[1])
    computed_output = computed_output + kind_weights[2] * (cond * field_sums[2] + accumulated_flux[2])
    return computed_output


def reference(opening_warmth_field, cellwise_warming_source, substance_category_per_voxel, thermal_coefficient_table, boundary_cooling_flags):
    cond = jnp.take(thermal_coefficient_table, substance_category_per_voxel)
    cond_sums = neighbor_sums(jnp.pad(cond, 1))
    spread = kind_weights[0] * (kind_counts[0] * cond + cond_sums[0])
    spread = spread + kind_weights[1] * (kind_counts[1] * cond + cond_sums[1])
    spread = spread + kind_weights[2] * (kind_counts[2] * cond + cond_sums[2])
    diagonal = 1.0 + interval_delta * cooling * boundary_cooling_flags.astype(jnp.float32) + 0.5 * interval_delta * spread

    def apply_stencil_matrix(field):
        padded = jnp.pad(field, 1)
        padded_flux = jnp.pad(cond * field, 1)
        return diagonal * field - 0.5 * interval_delta * coupling(padded, padded_flux, cond)

    closing_warmth_field = opening_warmth_field
    remaining_mismatch = opening_warmth_field
    for tstep in range(TSTEPS):
        forcing_term = closing_warmth_field + interval_delta * cellwise_warming_source
        remaining_mismatch = forcing_term - apply_stencil_matrix(closing_warmth_field)
        search_heading = remaining_mismatch
        norm_now = jnp.sum(remaining_mismatch * remaining_mismatch)
        for step in range(ITERS):
            image = apply_stencil_matrix(search_heading)
            descent_alpha = norm_now / jnp.sum(search_heading * image)
            closing_warmth_field = closing_warmth_field + descent_alpha * search_heading
            remaining_mismatch = remaining_mismatch - descent_alpha * image
            following_norm = jnp.sum(remaining_mismatch * remaining_mismatch)
            search_heading = remaining_mismatch + (following_norm / norm_now) * search_heading
            norm_now = following_norm
    return closing_warmth_field, remaining_mismatch
```

```python
import functools

import jax
import jax.numpy as jnp
from jax import lax
from jax.experimental import pallas as pl
from jax.experimental.pallas import tpu as pltpu
from jax.sharding import PartitionSpec as P

ITERS = 4
interval_delta = 2.0
cooling = 3.0

MESH = pl.DeviceIdType.MESH
AXES = ("gx", "gy", "gz")
SUB = 8
LANES = 128
FIELDS = 4
WARM, SOURCE, COND, FLAGS, EDGES = range(5)
SLOT = LANES // FIELDS
PAIRS = [(i, j) for i in range(ITERS + 1) for j in range(i, ITERS + 1) if i < ITERS]


def smooth(values, axis):
    size = values.shape[axis]
    once = values + pltpu.roll(values, 1, axis)
    return once + pltpu.roll(once, size - 1, axis)


def smooth_all(before, center, after):
    return smooth(smooth(before + (center + center) + after, 0), 1)


def kernel(
    counts,
    warm_in,
    source_in,
    category_in,
    table_in,
    flags_in,
    warm_out,
    left_out,
    grid,
    basis,
    flux,
    diag,
    table,
    ints,
    edges,
    beside,
    bound_row,
    bound_rows,
    gram_row,
    gram_rows,
    load_sems,
    raw_send,
    raw_recv,
    fwd_send,
    fwd_recv,
    z_send,
    z_recv,
    row_send,
    row_recv,
):
    devices = counts[0] * counts[1] * counts[2]
    nx, ny, nz = warm_out.shape
    depth = ITERS + 1
    wide, tall, long = grid.shape[1:]
    here = [lax.axis_index(a) for a in AXES]
    me = (here[0] * counts[1] + here[1]) * counts[2] + here[2]

    def at(linear):
        return {
            "gx": linear // (counts[1] * counts[2]),
            "gy": (linear // counts[2]) % counts[1],
            "gz": linear % counts[2],
        }

    main = (slice(depth, depth + nx), slice(0, ny), slice(0, nz))
    loads = [
        pltpu.make_async_copy(category_in, ints.at[0], load_sems.at[0]),
        pltpu.make_async_copy(flags_in, ints.at[1], load_sems.at[1]),
        pltpu.make_async_copy(
            warm_in, grid.at[WARM, pl.ds(depth, nx), pl.ds(0, ny), pl.ds(0, nz)], load_sems.at[2]
        ),
        pltpu.make_async_copy(
            source_in, grid.at[SOURCE, pl.ds(depth, nx), pl.ds(0, ny), pl.ds(0, nz)], load_sems.at[3]
        ),
    ]
    for load in loads[:2]:
        load.start()

    for f in range(FIELDS + 1):
        grid[f, 0:depth, :, 0:nz] = jnp.zeros((depth, tall, nz), jnp.float32)
        grid[f, depth + nx :, :, 0:nz] = jnp.zeros((depth, tall, nz), jnp.float32)
        grid[f, depth : depth + nx, ny:, 0:nz] = jnp.zeros((nx, tall - ny, nz), jnp.float32)
    beside[...] = jnp.zeros(beside.shape, jnp.float32)
    for load in loads[2:]:
        load.start()

    barrier = pltpu.get_barrier_semaphore()

    @pl.loop(1, devices)
    def _(step):
        pl.semaphore_signal(
            barrier, inc=1, device_id=at((me + step) % devices), device_id_type=MESH
        )

    for load in loads:
        load.wait()

    lookup = jnp.broadcast_to(table_in[...], (ny, LANES))
    lane = lax.broadcasted_iota(jnp.int32, (ny, LANES), 1)
    top = jnp.zeros((ny, LANES), jnp.float32)
    total = jnp.zeros((ny, LANES), jnp.float32)
    most = jnp.zeros((ny, LANES), jnp.float32)
    least = jnp.ones((ny, LANES), jnp.float32)
    for i in range(nx):
        cond = jnp.take_along_axis(lookup, ints[0, i], axis=1)
        flag = ints[1, i].astype(jnp.float32)
        grid[COND, depth + i, 0:ny, 0:nz] = cond
        grid[FLAGS, depth + i, 0:ny, 0:nz] = flag
        pieces = [
            grid[WARM, depth + i, 0:ny, 0:nz],
            grid[SOURCE, depth + i, 0:ny, 0:nz],
            cond,
            flag,
        ]
        packed = None
        for f, piece in enumerate(pieces):
            turned = pltpu.roll(piece, (f * SLOT + SLOT // 2) % LANES, 1)
            packed = turned if packed is None else jnp.where(lane // SLOT == f, turned, packed)
        edges[i] = packed
        top = jnp.maximum(top, cond)
        total = total + cond
        most = jnp.maximum(most, flag)
        least = jnp.minimum(least, flag)
    shrink = lambda op, v: op(op(v, axis=0, keepdims=True), axis=1, keepdims=True)
    mean = shrink(jnp.sum, total) * (1.0 / (nx * ny * nz))
    high = 1.0 + interval_delta * cooling * shrink(jnp.max, most)
    high = high + 8.0 * interval_delta * (shrink(jnp.max, top) + mean)
    low = 1.0 + interval_delta * cooling * shrink(jnp.min, least)
    row_lane = lax.broadcasted_iota(jnp.int32, (1, LANES), 1)
    row = jnp.where(row_lane == 0, high, -low)
    bound_row[...] = row
    bound_rows[me] = row

    pl.semaphore_wait(barrier, devices - 1)

    def remote(src, dst, send, recv, offset):
        return pltpu.make_async_remote_copy(
            src_ref=src,
            dst_ref=dst,
            send_sem=send,
            recv_sem=recv,
            device_id={a: here[k] + offset[k] for k, a in enumerate(AXES)},
            device_id_type=MESH,
        )

    def exists(offset):
        good = None
        for k in range(3):
            if offset[k] > 0:
                one = here[k] < counts[k] - 1
            elif offset[k] < 0:
                one = here[k] > 0
            else:
                continue
            good = one if good is None else jnp.logical_and(good, one)
        return good

    z_copies = []
    for k, dz in enumerate((1, -1)):
        copy = remote(edges, beside.at[k], z_send.at[k], z_recv.at[k], (0, 0, dz))
        z_copies.append((copy, dz))
        pl.when(exists((0, 0, dz)))(copy.start)

    def spread(row_ref, rows_ref, k):
        @pl.loop(1, devices)
        def _(step):
            pltpu.make_async_remote_copy(
                src_ref=row_ref,
                dst_ref=rows_ref.at[me],
                send_sem=row_send.at[k],
                recv_sem=row_recv.at[k],
                device_id=at((me + step) % devices),
                device_id_type=MESH,
            ).start()

    def spread_wait(rows_ref, k):
        whole = pltpu.make_async_remote_copy(
            src_ref=rows_ref.at[pl.ds(0, devices - 1)],
            dst_ref=rows_ref.at[pl.ds(0, devices - 1)],
            send_sem=row_send.at[k],
            recv_sem=row_recv.at[k],
            device_id=at((me + 1) % devices),
            device_id_type=MESH,
        )
        whole.wait_send()
        whole.wait_recv()

    if devices > 1:
        spread(bound_row, bound_rows, 0)

    def ranges(offset):
        dx, dy = offset
        if dx == 0:
            xs, xd, xn = depth, depth, nx
        elif dx > 0:
            xs, xd, xn = nx, 0, depth
        else:
            xs, xd, xn = depth, depth + nx, depth
        if dy == 0:
            ys, yd, yn = 0, 0, ny
        elif dy > 0:
            ys, yd, yn = ny - SUB, ny + SUB, SUB
        else:
            ys, yd, yn = 0, ny, SUB
        z = pl.ds(0, nz)
        return (pl.ds(xs, xn), pl.ds(ys, yn), z), (pl.ds(xd, xn), pl.ds(yd, yn), z)

    offsets = [(0, 1), (0, -1), (1, 1), (-1, -1), (1, -1), (-1, 1), (1, 0), (-1, 0)]

    def around(fields, sends, recvs):
        copies = []
        for k, offset in enumerate(offsets):
            src, dst = ranges(offset)
            copies.append(
                (
                    remote(
                        grid.at[(fields,) + src],
                        grid.at[(fields,) + dst],
                        sends.at[k],
                        recvs.at[k],
                        offset + (0,),
                    ),
                    offset,
                )
            )
        return copies

    raw = around(pl.ds(0, FIELDS), raw_send, raw_recv)
    fwd = around(pl.ds(EDGES, 1), fwd_send, fwd_recv)
    for copy, (dx, dy) in raw:
        pl.when(exists((dx, dy, 0)))(copy.start)

    for copy, dz in z_copies:
        pl.when(exists((0, 0, -dz)))(copy.wait_recv)
    low_half = lane % SLOT < SLOT // 2
    for i in range(nx):
        grid[EDGES, depth + i, 0:ny, 0:nz] = jnp.where(low_half, beside[0, i], beside[1, i])
    for copy, (dx, dy) in fwd:
        pl.when(exists((dx, dy, 0)))(copy.start)

    for copy, (dx, dy) in raw:
        pl.when(exists((-dx, -dy, 0)))(copy.wait_recv)
    for copy, (dx, dy) in fwd:
        pl.when(exists((-dx, -dy, 0)))(copy.wait_recv)

    for i in range(wide):
        packed = grid[EDGES, i, :, 0:nz]
        for f in range(FIELDS):
            grid[f, i, :, nz:] = pltpu.roll(packed, (-f * SLOT - SLOT // 2) % LANES, 1)
        flux[0, i] = grid[COND, i] * grid[WARM, i]

    if devices > 1:
        spread_wait(bound_rows, 0)
    bounds = jnp.max(bound_rows[...], axis=0)
    pick = lambda v, i: jnp.sum(jnp.where(row_lane == i, v, 0.0), axis=1, keepdims=True)
    high, low = pick(bounds, 0), -pick(bounds, 1)
    middle = 0.5 * (high + low)
    half = 0.5 * (high - low)
    scale = 1.0 / half

    def valid(index, size, k):
        inner = index < size
        right = jnp.logical_and(index < size + (SUB if k == 1 else LANES // 2), here[k] < counts[k] - 1)
        left = jnp.logical_and(index >= size + (SUB if k == 1 else LANES // 2), here[k] > 0)
        return jnp.logical_or(inner, jnp.logical_or(right, left))

    y_index = lax.broadcasted_iota(jnp.int32, (tall, long), 0)
    z_index = lax.broadcasted_iota(jnp.int32, (tall, long), 1)
    inside = jnp.where(
        jnp.logical_and(valid(y_index, ny, 1), valid(z_index, nz, 2)), 0.125 * interval_delta, 0.0
    )
    x_left = jnp.where(here[0] > 0, 1.0, 0.0)
    x_right = jnp.where(here[0] < counts[0] - 1, 1.0, 0.0)

    def mask(i):
        if i < depth:
            return inside * x_left
        if i >= depth + nx:
            return inside * x_right
        return inside

    quarter = 0.125 * interval_delta

    for i in range(1, wide - 1):
        cond = grid[COND, i]
        ring = smooth_all(grid[COND, i - 1], cond, grid[COND, i + 1])
        d = 1.0 + interval_delta * cooling * grid[FLAGS, i] + 8.0 * interval_delta * cond + quarter * ring
        diag[i] = d
        warm = grid[WARM, i]
        own = smooth_all(grid[WARM, i - 1], warm, grid[WARM, i + 1])
        push = smooth_all(flux[0, i - 1], flux[0, i], flux[0, i + 1])
        image = d * warm - (quarter * cond * own + mask(i) * push)
        left = warm + interval_delta * grid[SOURCE, i] - image
        basis[0, i] = left
        flux[1, i] = cond * left

    for k in range(ITERS):
        now, later = (k + 1) % 2, k % 2
        for i in range(2 + k, wide - 2 - k):
            cond = grid[COND, i]
            mid = basis[k, i]
            own = smooth_all(basis[k, i - 1], mid, basis[k, i + 1])
            push = smooth_all(flux[now, i - 1], flux[now, i], flux[now, i + 1])
            image = (diag[i] - middle) * mid - (quarter * cond * own + mask(i) * push)
            if k == 0:
                fresh = scale * image
            else:
                fresh = (2.0 * scale) * image - basis[k - 1, i]
            basis[k + 1, i] = fresh
            if k + 1 < ITERS:
                flux[later, i] = cond * fresh

    sums = [None] * len(PAIRS)
    for i in range(depth, depth + nx):
        rows = [basis[k, i, 0:ny, 0:nz] for k in range(ITERS + 1)]
        for n, (a, b) in enumerate(PAIRS):
            term = rows[a] * rows[b]
            sums[n] = term if sums[n] is None else sums[n] + term
    diagonal = lax.broadcasted_iota(jnp.int32, (SUB, LANES), 0)
    across = lax.broadcasted_iota(jnp.int32, (SUB, LANES), 1)
    row = jnp.zeros((SUB, LANES), jnp.float32)
    for start in range(0, len(PAIRS), SUB):
        tile = jnp.zeros((SUB, LANES), jnp.float32)
        for n in range(start, min(start + SUB, len(PAIRS))):
            tile = jnp.where(diagonal == n - start, jnp.sum(sums[n], axis=0, keepdims=True), tile)
        column = jnp.sum(tile, axis=1, keepdims=True)
        row = row + jnp.where(across == diagonal + start, column, 0.0)
    row = jnp.sum(row, axis=0, keepdims=True)
    gram_row[...] = row
    gram_rows[me] = row
    if devices > 1:
        spread(gram_row, gram_rows, 1)
        spread_wait(gram_rows, 1)
    row = jnp.sum(gram_rows[...], axis=0)
    gram = {}
    for n, (a, b) in enumerate(PAIRS):
        gram[a, b] = gram[b, a] = pick(row, n)

    def apply(p):
        q = [middle * a for a in p] + [None]
        q[len(p)] = jnp.zeros_like(half)
        for i, a in enumerate(p):
            if i == 0:
                q[1] = q[1] + half * a
            else:
                q[i + 1] = q[i + 1] + (0.5 * half) * a
                q[i - 1] = q[i - 1] + (0.5 * half) * a
        return q

    def product(p, q):
        value = None
        for i, a in enumerate(p):
            inner = None
            for j, b in enumerate(q):
                term = gram[i, j] * b
                inner = term if inner is None else inner + term
            inner = a * inner
            value = inner if value is None else value + inner
        return value

    left = [jnp.ones_like(half)]
    heading = list(left)
    moved = []
    norm = product(left, left)
    for step in range(ITERS):
        image = apply(heading)
        alpha = norm / product(heading, image)
        moved = [a + alpha * b for a, b in zip(moved, heading)] + [
            alpha * b for b in heading[len(moved) :]
        ]
        left = [a - alpha * b for a, b in zip(left, image)] + [
            -alpha * b for b in image[len(left) :]
        ]
        if step + 1 < ITERS:
            following = product(left, left)
            ratio = following / norm
            heading = [a + ratio * b for a, b in zip(left, heading)] + left[len(heading) :]
            norm = following

    for i in range(nx):
        warm = grid[WARM, depth + i, 0:ny, 0:nz]
        end = jnp.zeros_like(warm)
        for k in range(ITERS + 1):
            value = basis[k, depth + i, 0:ny, 0:nz]
            if k < ITERS:
                warm = warm + moved[k] * value
            end = end + left[k] * value
        warm_out[i] = warm
        left_out[i] = end

    for copy, dz in z_copies:
        pl.when(exists((0, 0, dz)))(copy.wait_send)
    for copy, (dx, dy) in raw + fwd:
        pl.when(exists((dx, dy, 0)))(copy.wait_send)


def body(counts, warm, source, category, table, flags):
    nx, ny, nz = warm.shape
    depth = ITERS + 1
    devices = counts[0] * counts[1] * counts[2]
    wide, tall, long = nx + 2 * depth, ny + 2 * SUB, nz + LANES
    table = jnp.pad(table, (0, LANES - table.shape[0]))[None]
    any_spec = pl.BlockSpec(memory_space=pl.ANY)
    vmem = pl.BlockSpec(memory_space=pltpu.VMEM)
    shape = jax.ShapeDtypeStruct(warm.shape, jnp.float32)
    f32 = jnp.float32
    return pl.pallas_call(
        functools.partial(kernel, counts),
        out_shape=(shape, shape),
        in_specs=[any_spec, any_spec, any_spec, vmem, any_spec],
        out_specs=(vmem, vmem),
        scratch_shapes=[
            pltpu.VMEM((FIELDS + 1, wide, tall, long), f32),
            pltpu.VMEM((ITERS + 1, wide, tall, long), f32),
            pltpu.VMEM((2, wide, tall, long), f32),
            pltpu.VMEM((wide, tall, long), f32),
            pltpu.VMEM((SUB, LANES), f32),
            pltpu.VMEM((2, nx, ny, nz), jnp.int32),
            pltpu.VMEM((nx, ny, nz), f32),
            pltpu.VMEM((2, nx, ny, nz), f32),
            pltpu.VMEM((1, LANES), f32),
            pltpu.VMEM((devices, 1, LANES), f32),
            pltpu.VMEM((1, LANES), f32),
            pltpu.VMEM((devices, 1, LANES), f32),
            pltpu.SemaphoreType.DMA((4,)),
            pltpu.SemaphoreType.DMA((8,)),
            pltpu.SemaphoreType.DMA((8,)),
            pltpu.SemaphoreType.DMA((8,)),
            pltpu.SemaphoreType.DMA((8,)),
            pltpu.SemaphoreType.DMA((2,)),
            pltpu.SemaphoreType.DMA((2,)),
            pltpu.SemaphoreType.DMA((2,)),
            pltpu.SemaphoreType.DMA((2,)),
        ],
        compiler_params=pltpu.CompilerParams(collective_id=0, has_side_effects=True),
    )(warm, source, category, table, flags)


def solution(mesh):
    counts = tuple(mesh.shape[a] for a in AXES)
    spec = P("gx", "gy", "gz")
    return jax.shard_map(
        functools.partial(body, counts),
        mesh=mesh,
        in_specs=(spec, spec, spec, P(), spec),
        out_specs=(spec, spec),
        check_vma=False,
    )
```

```python
import functools

import jax
import jax.numpy as jnp
from jax import lax
from jax.experimental import pallas as pl
from jax.experimental.pallas import tpu as pltpu
from jax.sharding import PartitionSpec as P

ITERS = 4
interval_delta = 2.0
cooling = 3.0

MESH = pl.DeviceIdType.MESH
AXES = ("gx", "gy", "gz")
SUB = 8
LANES = 128
FIELDS = 4
WARM, SOURCE, COND, FLAGS, EDGES = range(5)
SLOT = LANES // FIELDS
PAIRS = [(i, j) for i in range(ITERS + 1) for j in range(i, ITERS + 1) if i < ITERS]


def smooth(values, axis):
    size = values.shape[axis]
    return (values + values) + (pltpu.roll(values, 1, axis) + pltpu.roll(values, size - 1, axis))


def smooth_all(before, center, after):
    return smooth(smooth(before + (center + center) + after, 0), 1)


def kernel(
    counts,
    warm_in,
    source_in,
    category_in,
    table_in,
    flags_in,
    warm_out,
    left_out,
    grid,
    basis,
    flux,
    warm_flux,
    diag,
    couple,
    table,
    table_row,
    ints,
    edges,
    beside,
    row_out,
    plane_rows,
    line_rows,
    load_sems,
    raw_send,
    raw_recv,
    fwd_send,
    fwd_recv,
    z_send,
    z_recv,
    row_send,
    row_recv,
):
    plane, line = counts[0] * counts[1], counts[2]
    nx, ny, nz = warm_out.shape
    depth = ITERS + 1
    wide, tall, long = grid.shape[1:]
    short = ny + SUB
    here = [lax.axis_index(a) for a in AXES]
    in_plane = here[0] * counts[1] + here[1]
    plane_targets = [
        {"gx": other // counts[1], "gy": other % counts[1], "gz": here[2]}
        for other in [(in_plane + step) % plane for step in range(1, plane)]
    ]
    line_targets = [
        {"gx": here[0], "gy": here[1], "gz": (here[2] + step) % line} for step in range(1, line)
    ]

    loads = [
        pltpu.make_async_copy(category_in, ints.at[0], load_sems.at[0]),
        pltpu.make_async_copy(flags_in, ints.at[1], load_sems.at[1]),
        pltpu.make_async_copy(
            warm_in, grid.at[WARM, pl.ds(depth, nx), pl.ds(0, ny), pl.ds(0, nz)], load_sems.at[2]
        ),
        pltpu.make_async_copy(
            source_in, grid.at[SOURCE, pl.ds(depth, nx), pl.ds(0, ny), pl.ds(0, nz)], load_sems.at[3]
        ),
        pltpu.make_async_copy(table_in, table_row, load_sems.at[4]),
    ]
    for load in loads:
        load.start()

    for f in range(FIELDS + 1):
        grid[f, 0:depth, :, 0:nz] = jnp.zeros((depth, tall, nz), jnp.float32)
        grid[f, depth + nx :, :, 0:nz] = jnp.zeros((depth, tall, nz), jnp.float32)
        grid[f, depth : depth + nx, ny:, 0:nz] = jnp.zeros((nx, tall - ny, nz), jnp.float32)
    beside[...] = jnp.zeros(beside.shape, jnp.float32)
    table[...] = jnp.zeros(table.shape, jnp.float32)
    barrier = pltpu.get_barrier_semaphore()

    for target in plane_targets + line_targets:
        pl.semaphore_signal(barrier, inc=1, device_id=target, device_id_type=MESH)

    for load in loads:
        load.wait()

    table[0:1, 0 : table_in.shape[1]] = table_row[...]
    lookup = jnp.broadcast_to(table[0:1, :], (ny, LANES))
    lane = lax.broadcasted_iota(jnp.int32, (ny, LANES), 1)
    top = jnp.zeros((ny, LANES), jnp.float32)
    total = jnp.zeros((ny, LANES), jnp.float32)
    most = jnp.zeros((ny, LANES), jnp.float32)
    least = jnp.ones((ny, LANES), jnp.float32)
    for i in range(nx):
        cond = jnp.take_along_axis(lookup, ints[0, i], axis=1)
        flag = ints[1, i].astype(jnp.float32)
        grid[COND, depth + i, 0:ny, 0:nz] = cond
        grid[FLAGS, depth + i, 0:ny, 0:nz] = flag
        pieces = [
            grid[WARM, depth + i, 0:ny, 0:nz],
            grid[SOURCE, depth + i, 0:ny, 0:nz],
            cond,
            flag,
        ]
        packed = None
        for f, piece in enumerate(pieces):
            turned = pltpu.roll(piece, (f * SLOT + SLOT // 2) % LANES, 1)
            packed = turned if packed is None else jnp.where(lane // SLOT == f, turned, packed)
        edges[i] = packed
        top = jnp.maximum(top, cond)
        total = total + cond
        most = jnp.maximum(most, flag)
        least = jnp.minimum(least, flag)
    shrink = lambda op, v: op(op(v, axis=0, keepdims=True), axis=1, keepdims=True)
    mean = shrink(jnp.sum, total) * (1.0 / (nx * ny * nz))
    high = 1.0 + interval_delta * cooling * shrink(jnp.max, most)
    high = high + 8.0 * interval_delta * (shrink(jnp.max, top) + mean)
    low = 1.0 + interval_delta * cooling * shrink(jnp.min, least)
    row_lane = lax.broadcasted_iota(jnp.int32, (1, LANES), 1)
    row = jnp.where(row_lane == 0, high, -low)
    row_out[0] = row
    plane_rows[0, in_plane] = row

    pl.semaphore_wait(barrier, plane + line - 2)

    def remote(src, dst, send, recv, offset):
        return pltpu.make_async_remote_copy(
            src_ref=src,
            dst_ref=dst,
            send_sem=send,
            recv_sem=recv,
            device_id={a: here[k] + offset[k] for k, a in enumerate(AXES)},
            device_id_type=MESH,
        )

    def exists(offset):
        good = None
        for k in range(3):
            if offset[k] > 0:
                one = here[k] < counts[k] - 1
            elif offset[k] < 0:
                one = here[k] > 0
            else:
                continue
            good = one if good is None else jnp.logical_and(good, one)
        return good

    z_copies = []
    for k, dz in enumerate((1, -1)):
        copy = remote(edges, beside.at[k], z_send.at[k], z_recv.at[k], (0, 0, dz))
        z_copies.append((copy, dz))
        pl.when(exists((0, 0, dz)))(copy.start)

    def share(stage, rows_ref, slot, targets):
        for target in targets:
            pltpu.make_async_remote_copy(
                src_ref=row_out.at[stage],
                dst_ref=rows_ref.at[slot],
                send_sem=row_send.at[stage],
                recv_sem=row_recv.at[stage],
                device_id=target,
                device_id_type=MESH,
            ).start()

    def share_wait(stage, rows_ref, targets):
        if targets:
            whole = pltpu.make_async_remote_copy(
                src_ref=rows_ref.at[pl.ds(0, len(targets))],
                dst_ref=rows_ref.at[pl.ds(0, len(targets))],
                send_sem=row_send.at[stage],
                recv_sem=row_recv.at[stage],
                device_id=targets[0],
                device_id_type=MESH,
            )
            whole.wait_send()
            whole.wait_recv()

    def ranges(offset):
        dx, dy = offset
        if dx == 0:
            xs, xd, xn = depth, depth, nx
        elif dx > 0:
            xs, xd, xn = nx, 0, depth
        else:
            xs, xd, xn = depth, depth + nx, depth
        if dy == 0:
            ys, yd, yn = 0, 0, ny
        elif dy > 0:
            ys, yd, yn = ny - SUB, ny + SUB, SUB
        else:
            ys, yd, yn = 0, ny, SUB
        z = pl.ds(0, nz)
        return (pl.ds(xs, xn), pl.ds(ys, yn), z), (pl.ds(xd, xn), pl.ds(yd, yn), z)

    offsets = [(0, 1), (0, -1), (1, 1), (-1, -1), (1, -1), (-1, 1), (1, 0), (-1, 0)]

    def around(fields, sends, recvs):
        copies = []
        for k, offset in enumerate(offsets):
            src, dst = ranges(offset)
            copies.append(
                (
                    remote(
                        grid.at[(fields,) + src],
                        grid.at[(fields,) + dst],
                        sends.at[k],
                        recvs.at[k],
                        offset + (0,),
                    ),
                    offset,
                )
            )
        return copies

    raw = around(pl.ds(0, FIELDS), raw_send, raw_recv)
    fwd = around(pl.ds(EDGES, 1), fwd_send, fwd_recv)
    for copy, (dx, dy) in raw:
        pl.when(exists((dx, dy, 0)))(copy.start)

    share(0, plane_rows.at[0], in_plane, plane_targets)

    for copy, dz in z_copies:
        pl.when(exists((0, 0, -dz)))(copy.wait_recv)
    low_half = lane % SLOT < SLOT // 2
    for i in range(nx):
        grid[EDGES, depth + i, 0:ny, 0:nz] = jnp.where(low_half, beside[0, i], beside[1, i])
    for copy, (dx, dy) in fwd:
        pl.when(exists((dx, dy, 0)))(copy.start)

    share_wait(0, plane_rows.at[0], plane_targets)
    row = jnp.max(plane_rows[0], axis=0)
    row_out[1] = row
    line_rows[0, here[2]] = row
    share(1, line_rows.at[0], here[2], line_targets)

    for copy, (dx, dy) in raw:
        pl.when(exists((-dx, -dy, 0)))(copy.wait_recv)
    for copy, (dx, dy) in fwd:
        pl.when(exists((-dx, -dy, 0)))(copy.wait_recv)

    @pl.loop(0, wide // 2)
    def _(pair):
        for u in range(2):
            i = 2 * pair + u
            packed = grid[EDGES, i, :, 0:nz]
            for f in range(FIELDS):
                grid[f, i, :, nz:] = pltpu.roll(packed, (-f * SLOT - SLOT // 2) % LANES, 1)
            warm_flux[i] = grid[COND, i] * grid[WARM, i]

    share_wait(1, line_rows.at[0], line_targets)
    bounds = jnp.max(line_rows[0], axis=0)
    pick = lambda v, i: jnp.sum(jnp.where(row_lane == i, v, 0.0), axis=1, keepdims=True)
    high, low = pick(bounds, 0), -pick(bounds, 1)
    middle = 0.5 * (high + low)
    half = 0.5 * (high - low)
    twice = 2.0 / half

    def valid(index, size, cut, k):
        inner = index < size
        right = jnp.logical_and(index < size + cut, here[k] < counts[k] - 1)
        left = jnp.logical_and(index >= size + cut, here[k] > 0)
        return jnp.logical_or(inner, jnp.logical_or(right, left))

    def inside_of(rows, cut):
        y_index = lax.broadcasted_iota(jnp.int32, (rows, long), 0)
        z_index = lax.broadcasted_iota(jnp.int32, (rows, long), 1)
        both = jnp.logical_and(valid(y_index, ny, cut, 1), valid(z_index, nz, LANES // 2, 2))
        return jnp.where(both, 1.0, 0.0)

    x_left = jnp.where(here[0] > 0, 1.0, 0.0)
    x_right = jnp.where(here[0] < counts[0] - 1, 1.0, 0.0)

    def x_inside(i):
        return jnp.where(i < depth, x_left, jnp.where(i >= depth + nx, x_right, 1.0))

    quarter = 0.125 * interval_delta
    inside = quarter * inside_of(tall, SUB)
    first_half = lax.broadcasted_iota(jnp.int32, (SUB, long), 0) < SUB // 2

    def narrow(v):
        ends = jnp.where(first_half, v[ny : ny + SUB], v[ny + SUB :])
        return jnp.concatenate([v[:ny], ends], axis=0)

    @pl.loop(0, (wide - 2) // 2)
    def _(pair):
        for u in range(2):
            i = 1 + 2 * pair + u
            cond = grid[COND, i]
            ring = smooth_all(grid[COND, i - 1], cond, grid[COND, i + 1])
            d = 1.0 + interval_delta * cooling * grid[FLAGS, i]
            d = d + 8.0 * interval_delta * cond + quarter * ring
            warm = grid[WARM, i]
            own = smooth_all(grid[WARM, i - 1], warm, grid[WARM, i + 1])
            push = smooth_all(warm_flux[i - 1], warm_flux[i], warm_flux[i + 1])
            image = d * warm - (quarter * cond * own + x_inside(i) * inside * push)
            left = narrow(warm + interval_delta * grid[SOURCE, i] - image)
            edge = (quarter * twice) * narrow(cond)
            basis[0, i] = left
            diag[i] = twice * (narrow(d) - middle)
            couple[i] = edge
            flux[0, i] = edge * left

    within = inside_of(short, SUB // 2)
    for k in range(ITERS):

        @pl.loop(0, (wide - 4 - 2 * k) // 2)
        def _(pair):
            for u in range(2):
                i = 2 + k + 2 * pair + u
                edge = couple[i]
                mid = basis[k, i]
                own = smooth_all(basis[k, i - 1], mid, basis[k, i + 1])
                push = smooth_all(flux[k % 2, i - 1], flux[k % 2, i], flux[k % 2, i + 1])
                fresh = diag[i] * mid - (edge * own + x_inside(i) * within * push)
                if k > 0:
                    fresh = fresh - basis[k - 1, i]
                basis[k + 1, i] = fresh
                if k + 1 < ITERS:
                    flux[(k + 1) % 2, i] = edge * fresh

    sums = [None] * len(PAIRS)
    for i in range(depth, depth + nx):
        rows = [basis[k, i, 0:ny, 0:nz] for k in range(ITERS + 1)]
        for n, (a, b) in enumerate(PAIRS):
            term = rows[a] * rows[b]
            sums[n] = term if sums[n] is None else sums[n] + term
    diagonal = lax.broadcasted_iota(jnp.int32, (SUB, LANES), 0)
    across = lax.broadcasted_iota(jnp.int32, (SUB, LANES), 1)
    row = jnp.zeros((SUB, LANES), jnp.float32)
    for start in range(0, len(PAIRS), SUB):
        tile = jnp.zeros((SUB, LANES), jnp.float32)
        for n in range(start, min(start + SUB, len(PAIRS))):
            tile = jnp.where(diagonal == n - start, jnp.sum(sums[n], axis=0, keepdims=True), tile)
        column = jnp.sum(tile, axis=1, keepdims=True)
        row = row + jnp.where(across == diagonal + start, column, 0.0)
    row = jnp.sum(row, axis=0, keepdims=True)
    row_out[2] = row
    plane_rows[1, in_plane] = row
    share(2, plane_rows.at[1], in_plane, plane_targets)
    share_wait(2, plane_rows.at[1], plane_targets)
    row = jnp.sum(plane_rows[1], axis=0)
    row_out[3] = row
    line_rows[1, here[2]] = row
    share(3, line_rows.at[1], here[2], line_targets)
    share_wait(3, line_rows.at[1], line_targets)
    row = jnp.sum(line_rows[1], axis=0)
    gram = {}
    for n, (a, b) in enumerate(PAIRS):
        gram[a, b] = gram[b, a] = pick(row, n)

    def apply(p):
        q = [middle * a for a in p] + [jnp.zeros_like(half)]
        for i, a in enumerate(p):
            q[i + 1] = q[i + 1] + (0.5 * half) * a
            if i > 0:
                q[i - 1] = q[i - 1] + (0.5 * half) * a
        return q

    def product(p, q):
        value = None
        for i, a in enumerate(p):
            inner = None
            for j, b in enumerate(q):
                term = gram[i, j] * b
                inner = term if inner is None else inner + term
            inner = a * inner
            value = inner if value is None else value + inner
        return value

    left = [jnp.ones_like(half)]
    heading = list(left)
    moved = []
    norm = product(left, left)
    for step in range(ITERS):
        image = apply(heading)
        alpha = norm / product(heading, image)
        moved = [a + alpha * b for a, b in zip(moved, heading)] + [
            alpha * b for b in heading[len(moved) :]
        ]
        left = [a - alpha * b for a, b in zip(left, image)] + [
            -alpha * b for b in image[len(left) :]
        ]
        if step + 1 < ITERS:
            following = product(left, left)
            ratio = following / norm
            heading = [a + ratio * b for a, b in zip(left, heading)] + left[len(heading) :]
            norm = following

    for i in range(nx):
        warm = grid[WARM, depth + i, 0:ny, 0:nz]
        end = jnp.zeros_like(warm)
        for k in range(ITERS + 1):
            value = basis[k, depth + i, 0:ny, 0:nz]
            if k < ITERS:
                warm = warm + moved[k] * value
            end = end + left[k] * value
        warm_out[i] = warm
        left_out[i] = end

    for copy, dz in z_copies:
        pl.when(exists((0, 0, dz)))(copy.wait_send)
    for copy, (dx, dy) in raw + fwd:
        pl.when(exists((dx, dy, 0)))(copy.wait_send)


def body(counts, warm, source, category, table, flags):
    nx, ny, nz = warm.shape
    depth = ITERS + 1
    plane, line = counts[0] * counts[1], counts[2]
    if nx < depth or nx % 2 or ny % SUB or nz != LANES or table.shape[0] > LANES:
        raise ValueError("block shape")
    wide, tall, short, long = nx + 2 * depth, ny + 2 * SUB, ny + SUB, nz + LANES
    table = table[None]
    any_spec = pl.BlockSpec(memory_space=pl.ANY)
    vmem = pl.BlockSpec(memory_space=pltpu.VMEM)
    shape = jax.ShapeDtypeStruct(warm.shape, jnp.float32)
    f32 = jnp.float32
    return pl.pallas_call(
        functools.partial(kernel, counts),
        out_shape=(shape, shape),
        in_specs=[any_spec] * 5,
        out_specs=(vmem, vmem),
        scratch_shapes=[
            pltpu.VMEM((FIELDS + 1, wide, tall, long), f32),
            pltpu.VMEM((ITERS + 1, wide, short, long), f32),
            pltpu.VMEM((2, wide, short, long), f32),
            pltpu.VMEM((wide, tall, long), f32),
            pltpu.VMEM((wide, short, long), f32),
            pltpu.VMEM((wide, short, long), f32),
            pltpu.VMEM((SUB, LANES), f32),
            pltpu.VMEM(table.shape, f32),
            pltpu.VMEM((2, nx, ny, nz), jnp.int32),
            pltpu.VMEM((nx, ny, nz), f32),
            pltpu.VMEM((2, nx, ny, nz), f32),
            pltpu.VMEM((4, 1, LANES), f32),
            pltpu.VMEM((2, plane, 1, LANES), f32),
            pltpu.VMEM((2, line, 1, LANES), f32),
            pltpu.SemaphoreType.DMA((5,)),
            pltpu.SemaphoreType.DMA((8,)),
            pltpu.SemaphoreType.DMA((8,)),
            pltpu.SemaphoreType.DMA((8,)),
            pltpu.SemaphoreType.DMA((8,)),
            pltpu.SemaphoreType.DMA((2,)),
            pltpu.SemaphoreType.DMA((2,)),
            pltpu.SemaphoreType.DMA((4,)),
            pltpu.SemaphoreType.DMA((4,)),
        ],
        compiler_params=pltpu.CompilerParams(collective_id=0, has_side_effects=True),
    )(warm, source, category, table, flags)


def solution(mesh):
    counts = tuple(mesh.shape[a] for a in AXES)
    spec = P("gx", "gy", "gz")
    return jax.shard_map(
        functools.partial(body, counts),
        mesh=mesh,
        in_specs=(spec, spec, spec, P(), spec),
        out_specs=(spec, spec),
        check_vma=False,
    )
```

```python
import functools

import jax
import jax.numpy as jnp
from jax import lax
from jax.experimental import pallas as pl
from jax.experimental.pallas import tpu as pltpu
from jax.sharding import PartitionSpec as P

ITERS = 4
interval_delta = 2.0
cooling = 3.0

MESH = pl.DeviceIdType.MESH
AXES = ("gx", "gy", "gz")
SUB = 8
DIRECT = 64
LANES = 128
FIELDS = 4
WARM, COND, SOURCE, FLAGS, EDGES = range(5)
SLOT = LANES // FIELDS
PAIRS = [(i, j) for i in range(ITERS + 1) for j in range(i, ITERS + 1) if i < ITERS]


def smooth(values, axis):
    size = values.shape[axis]
    return (values + values) + (pltpu.roll(values, 1, axis) + pltpu.roll(values, size - 1, axis))


def smooth_all(before, center, after):
    return smooth(smooth(before + (center + center) + after, 0), 1)


def kernel(
    counts,
    warm_in,
    source_in,
    category_in,
    table_in,
    flags_in,
    warm_out,
    left_out,
    grid,
    basis,
    flux,
    warm_flux,
    diag,
    couple,
    table,
    table_row,
    ints,
    edges,
    mixed,
    beside,
    row_out,
    plane_rows,
    line_rows,
    all_rows,
    load_sems,
    raw_send,
    raw_recv,
    mix_send,
    mix_recv,
    fwd_send,
    fwd_recv,
    z_send,
    z_recv,
    row_send,
    row_recv,
):
    plane, line = counts[0] * counts[1], counts[2]
    nx, ny, nz = warm_out.shape
    depth = ITERS + 1
    wide, tall, long = grid.shape[1:]
    short = ny + SUB
    here = [lax.axis_index(a) for a in AXES]
    in_plane = here[0] * counts[1] + here[1]
    plane_targets = [
        {"gx": other // counts[1], "gy": other % counts[1], "gz": here[2]}
        for other in [(in_plane + step) % plane for step in range(1, plane)]
    ]
    line_targets = [
        {"gx": here[0], "gy": here[1], "gz": (here[2] + step) % line} for step in range(1, line)
    ]

    loads = [
        pltpu.make_async_copy(category_in, ints.at[0], load_sems.at[0]),
        pltpu.make_async_copy(flags_in, ints.at[1], load_sems.at[1]),
        pltpu.make_async_copy(
            warm_in, grid.at[WARM, pl.ds(depth, nx), pl.ds(0, ny), pl.ds(0, nz)], load_sems.at[2]
        ),
        pltpu.make_async_copy(
            source_in, grid.at[SOURCE, pl.ds(depth, nx), pl.ds(0, ny), pl.ds(0, nz)], load_sems.at[3]
        ),
        pltpu.make_async_copy(table_in, table_row, load_sems.at[4]),
    ]
    for load in loads:
        load.start()

    for f in range(FIELDS + 1):
        grid[f, 0:depth, :, 0:nz] = jnp.zeros((depth, tall, nz), jnp.float32)
        grid[f, depth + nx :, :, 0:nz] = jnp.zeros((depth, tall, nz), jnp.float32)
        grid[f, depth : depth + nx, ny:, 0:nz] = jnp.zeros((nx, tall - ny, nz), jnp.float32)
    beside[...] = jnp.zeros(beside.shape, jnp.float32)
    table[...] = jnp.zeros(table.shape, jnp.float32)
    moved_by = [[(here[k] + step) % counts[k] for step in range(counts[k])] for k in range(3)]
    all_targets = [
        {"gx": moved_by[0][a], "gy": moved_by[1][b], "gz": moved_by[2][c]}
        for c in reversed(range(counts[2]))
        for b in reversed(range(counts[1]))
        for a in reversed(range(counts[0]))
        if a or b or c
    ]

    barrier = pltpu.get_barrier_semaphore()

    for target in plane_targets + line_targets:
        pl.semaphore_signal(barrier, inc=1, device_id=target, device_id_type=MESH)

    for load in loads:
        load.wait()

    table[0:1, 0 : table_in.shape[1]] = table_row[...]
    lookup = jnp.broadcast_to(table[0:1, :], (ny, LANES))
    lane = lax.broadcasted_iota(jnp.int32, (ny, LANES), 1)
    top = jnp.zeros((ny, LANES), jnp.float32)
    total = jnp.zeros((ny, LANES), jnp.float32)
    most = jnp.zeros((ny, LANES), jnp.float32)
    least = jnp.ones((ny, LANES), jnp.float32)
    for i in range(nx):
        cond = jnp.take_along_axis(lookup, ints[0, i], axis=1)
        flag = ints[1, i].astype(jnp.float32)
        grid[COND, depth + i, 0:ny, 0:nz] = cond
        grid[FLAGS, depth + i, 0:ny, 0:nz] = flag
        pieces = [
            grid[WARM, depth + i, 0:ny, 0:nz],
            cond,
            grid[SOURCE, depth + i, 0:ny, 0:nz],
            flag,
        ]
        packed = None
        for f, piece in enumerate(pieces):
            turned = pltpu.roll(piece, (f * SLOT + SLOT // 2) % LANES, 1)
            packed = turned if packed is None else jnp.where(lane // SLOT == f, turned, packed)
        edges[i] = packed
        upper = lax.broadcasted_iota(jnp.int32, (SUB, nz), 0) < SUB // 2
        last, first = slice(ny - SUB, ny), slice(0, SUB)
        mixed[0, i] = jnp.where(
            upper, pltpu.roll(flag[last], SUB // 2, 0), grid[SOURCE, depth + i, last, 0:nz]
        )
        mixed[1, i] = jnp.where(
            upper, grid[SOURCE, depth + i, first, 0:nz], pltpu.roll(flag[first], SUB // 2, 0)
        )
        top = jnp.maximum(top, cond)
        total = total + cond
        most = jnp.maximum(most, flag)
        least = jnp.minimum(least, flag)
    shrink = lambda op, v: op(op(v, axis=0, keepdims=True), axis=1, keepdims=True)
    mean = shrink(jnp.sum, total) * (1.0 / (nx * ny * nz))
    high = 1.0 + interval_delta * cooling * shrink(jnp.max, most)
    high = high + 8.0 * interval_delta * (shrink(jnp.max, top) + mean)
    low = 1.0 + interval_delta * cooling * shrink(jnp.min, least)
    row_lane = lax.broadcasted_iota(jnp.int32, (1, LANES), 1)
    row = jnp.where(row_lane == 0, high, -low)
    row_out[0] = row
    plane_rows[0, in_plane] = row

    pl.semaphore_wait(barrier, plane + line - 2)

    def remote(src, dst, send, recv, offset):
        return pltpu.make_async_remote_copy(
            src_ref=src,
            dst_ref=dst,
            send_sem=send,
            recv_sem=recv,
            device_id={a: here[k] + offset[k] for k, a in enumerate(AXES)},
            device_id_type=MESH,
        )

    def exists(offset):
        good = None
        for k in range(3):
            if offset[k] > 0:
                one = here[k] < counts[k] - 1
            elif offset[k] < 0:
                one = here[k] > 0
            else:
                continue
            good = one if good is None else jnp.logical_and(good, one)
        return good

    z_copies = []
    for k, dz in enumerate((1, -1)):
        copy = remote(edges, beside.at[k], z_send.at[k], z_recv.at[k], (0, 0, dz))
        z_copies.append((copy, dz))
        pl.when(exists((0, 0, dz)))(copy.start)

    def share(stage, rows_ref, slot, targets):
        for target in targets:
            pltpu.make_async_remote_copy(
                src_ref=row_out.at[stage],
                dst_ref=rows_ref.at[slot],
                send_sem=row_send.at[stage],
                recv_sem=row_recv.at[stage],
                device_id=target,
                device_id_type=MESH,
            ).start()

    def share_wait(stage, rows_ref, targets):
        if targets:
            whole = pltpu.make_async_remote_copy(
                src_ref=rows_ref.at[pl.ds(0, len(targets))],
                dst_ref=rows_ref.at[pl.ds(0, len(targets))],
                send_sem=row_send.at[stage],
                recv_sem=row_recv.at[stage],
                device_id=targets[0],
                device_id_type=MESH,
            )
            whole.wait_send()
            whole.wait_recv()

    def ranges(offset):
        dx, dy = offset
        if dx == 0:
            xs, xd, xn = depth, depth, nx
        elif dx > 0:
            xs, xd, xn = nx, 0, depth
        else:
            xs, xd, xn = depth, depth + nx, depth
        if dy == 0:
            ys, yd, yn = 0, 0, ny
        elif dy > 0:
            ys, yd, yn = ny - SUB, ny + SUB, SUB
        else:
            ys, yd, yn = 0, ny, SUB
        z = pl.ds(0, nz)
        return (pl.ds(xs, xn), pl.ds(ys, yn), z), (pl.ds(xd, xn), pl.ds(yd, yn), z)

    offsets = [(0, 1), (0, -1), (1, 1), (-1, -1), (1, -1), (-1, 1), (1, 0), (-1, 0)]

    raw, fwd = [], []
    for k, offset in enumerate(offsets):
        src, dst = ranges(offset)
        full = offset + (0,)
        count = FIELDS if offset[1] == 0 else SOURCE
        fields = (pl.ds(0, count),)
        raw.append(
            (
                remote(
                    grid.at[fields + src], grid.at[fields + dst], raw_send.at[k], raw_recv.at[k], full
                ),
                offset,
            )
        )
        if offset[1] != 0:
            xs = pl.ds(src[0].start - depth, src[0].size)
            raw.append(
                (
                    remote(
                        mixed.at[0 if offset[1] > 0 else 1, xs],
                        grid.at[(SOURCE,) + dst],
                        mix_send.at[k],
                        mix_recv.at[k],
                        full,
                    ),
                    offset,
                )
            )
        fwd.append(
            (
                remote(
                    grid.at[(EDGES,) + src], grid.at[(EDGES,) + dst], fwd_send.at[k], fwd_recv.at[k], full
                ),
                offset,
            )
        )
    for copy, (dx, dy) in raw:
        pl.when(exists((dx, dy, 0)))(copy.start)

    share(0, plane_rows.at[0], in_plane, plane_targets)

    for copy, dz in z_copies:
        pl.when(exists((0, 0, -dz)))(copy.wait_recv)
    low_half = lane % SLOT < SLOT // 2
    for i in range(nx):
        grid[EDGES, depth + i, 0:ny, 0:nz] = jnp.where(low_half, beside[0, i], beside[1, i])
    for copy, (dx, dy) in fwd:
        pl.when(exists((dx, dy, 0)))(copy.start)

    share_wait(0, plane_rows.at[0], plane_targets)
    row = jnp.max(plane_rows[0], axis=0)
    row_out[1] = row
    line_rows[0, here[2]] = row
    share(1, line_rows.at[0], here[2], line_targets)

    for copy, (dx, dy) in raw:
        pl.when(exists((-dx, -dy, 0)))(copy.wait_recv)
    for copy, (dx, dy) in fwd:
        pl.when(exists((-dx, -dy, 0)))(copy.wait_recv)

    batch = next(u for u in (6, 4, 2) if wide % u == 0)

    @pl.loop(0, wide // batch)
    def _(group):
        for u in range(batch):
            i = batch * group + u
            packed = grid[EDGES, i, :, 0:nz]
            grid[FLAGS, i, ny:, 0:nz] = jnp.concatenate(
                [
                    pltpu.roll(grid[SOURCE, i, ny : ny + SUB, 0:nz], SUB // 2, 0),
                    pltpu.roll(grid[SOURCE, i, ny + SUB :, 0:nz], SUB // 2, 0),
                ],
                axis=0,
            )
            for f in range(FIELDS):
                grid[f, i, :, nz:] = pltpu.roll(packed, (-f * SLOT - SLOT // 2) % LANES, 1)
            warm_flux[i] = grid[COND, i] * grid[WARM, i]

    share_wait(1, line_rows.at[0], line_targets)
    bounds = jnp.max(line_rows[0], axis=0)
    pick = lambda v, i: jnp.sum(jnp.where(row_lane == i, v, 0.0), axis=1, keepdims=True)
    high, low = pick(bounds, 0), -pick(bounds, 1)
    middle = 0.5 * (high + low)
    half = 0.5 * (high - low)
    twice = 2.0 / half

    def valid(index, size, cut, k):
        inner = index < size
        right = jnp.logical_and(index < size + cut, here[k] < counts[k] - 1)
        left = jnp.logical_and(index >= size + cut, here[k] > 0)
        return jnp.logical_or(inner, jnp.logical_or(right, left))

    def inside_of(rows, cut):
        y_index = lax.broadcasted_iota(jnp.int32, (rows, long), 0)
        z_index = lax.broadcasted_iota(jnp.int32, (rows, long), 1)
        both = jnp.logical_and(valid(y_index, ny, cut, 1), valid(z_index, nz, LANES // 2, 2))
        return jnp.where(both, 1.0, 0.0)

    x_left = jnp.where(here[0] > 0, 1.0, 0.0)
    x_right = jnp.where(here[0] < counts[0] - 1, 1.0, 0.0)

    def x_inside(i):
        return jnp.where(i < depth, x_left, jnp.where(i >= depth + nx, x_right, 1.0))

    quarter = 0.125 * interval_delta
    inside = quarter * inside_of(tall, SUB)
    first_half = lax.broadcasted_iota(jnp.int32, (SUB, long), 0) < SUB // 2

    def narrow(v):
        ends = jnp.where(first_half, v[ny : ny + SUB], v[ny + SUB :])
        return jnp.concatenate([v[:ny], ends], axis=0)

    several = next(u for u in (4, 2) if (wide - 2) % u == 0)

    @pl.loop(0, (wide - 2) // several)
    def _(group):
        for u in range(several):
            i = 1 + several * group + u
            cond = grid[COND, i]
            ring = smooth_all(grid[COND, i - 1], cond, grid[COND, i + 1])
            d = 1.0 + interval_delta * cooling * grid[FLAGS, i]
            d = d + 8.0 * interval_delta * cond + quarter * ring
            warm = grid[WARM, i]
            own = smooth_all(grid[WARM, i - 1], warm, grid[WARM, i + 1])
            push = smooth_all(warm_flux[i - 1], warm_flux[i], warm_flux[i + 1])
            image = d * warm - (quarter * cond * own + x_inside(i) * inside * push)
            left = narrow(warm + interval_delta * grid[SOURCE, i] - image)
            edge = (quarter * twice) * narrow(cond)
            basis[0, i] = left
            diag[i] = twice * (narrow(d) - middle)
            couple[i] = edge
            flux[0, i] = edge * left

    within = inside_of(short, SUB // 2)
    for k in range(ITERS):

        half_planes = wide // 2 - 2 - k

        @pl.loop(0, 2)
        def _(group):
            for u in range(half_planes):
                i = 2 + k + half_planes * group + u
                edge = couple[i]
                mid = basis[k, i]
                own = smooth_all(basis[k, i - 1], mid, basis[k, i + 1])
                push = smooth_all(flux[k % 2, i - 1], flux[k % 2, i], flux[k % 2, i + 1])
                fresh = diag[i] * mid - (edge * own + x_inside(i) * within * push)
                if k > 0:
                    fresh = fresh - basis[k - 1, i]
                basis[k + 1, i] = fresh
                if k + 1 < ITERS:
                    flux[(k + 1) % 2, i] = edge * fresh

    sums = [None] * len(PAIRS)
    for i in range(depth, depth + nx):
        rows = [basis[k, i, 0:ny, 0:nz] for k in range(ITERS + 1)]
        for n, (a, b) in enumerate(PAIRS):
            term = rows[a] * rows[b]
            sums[n] = term if sums[n] is None else sums[n] + term
    diagonal = lax.broadcasted_iota(jnp.int32, (SUB, LANES), 0)
    across = lax.broadcasted_iota(jnp.int32, (SUB, LANES), 1)
    row = jnp.zeros((SUB, LANES), jnp.float32)
    for start in range(0, len(PAIRS), SUB):
        tile = jnp.zeros((SUB, LANES), jnp.float32)
        for n in range(start, min(start + SUB, len(PAIRS))):
            tile = jnp.where(diagonal == n - start, jnp.sum(sums[n], axis=0, keepdims=True), tile)
        column = jnp.sum(tile, axis=1, keepdims=True)
        row = row + jnp.where(across == diagonal + start, column, 0.0)
    row = jnp.sum(row, axis=0, keepdims=True)
    row_out[2] = row
    if plane * line <= DIRECT:
        mine = in_plane * line + here[2]
        all_rows[mine] = row
        share(2, all_rows, mine, all_targets)
        share_wait(2, all_rows, all_targets)
        row = jnp.sum(all_rows[...], axis=0)
    else:
        plane_rows[1, in_plane] = row
        share(2, plane_rows.at[1], in_plane, plane_targets)
        share_wait(2, plane_rows.at[1], plane_targets)
        row = jnp.sum(plane_rows[1], axis=0)
        row_out[3] = row
        line_rows[1, here[2]] = row
        share(3, line_rows.at[1], here[2], line_targets)
        share_wait(3, line_rows.at[1], line_targets)
        row = jnp.sum(line_rows[1], axis=0)
    gram = {}
    for n, (a, b) in enumerate(PAIRS):
        gram[a, b] = gram[b, a] = pick(row, n)

    def apply(p):
        q = [middle * a for a in p] + [jnp.zeros_like(half)]
        for i, a in enumerate(p):
            q[i + 1] = q[i + 1] + (0.5 * half) * a
            if i > 0:
                q[i - 1] = q[i - 1] + (0.5 * half) * a
        return q

    def product(p, q):
        value = None
        for i, a in enumerate(p):
            inner = None
            for j, b in enumerate(q):
                term = gram[i, j] * b
                inner = term if inner is None else inner + term
            inner = a * inner
            value = inner if value is None else value + inner
        return value

    left = [jnp.ones_like(half)]
    heading = list(left)
    moved = []
    norm = product(left, left)
    for step in range(ITERS):
        image = apply(heading)
        alpha = norm / product(heading, image)
        moved = [a + alpha * b for a, b in zip(moved, heading)] + [
            alpha * b for b in heading[len(moved) :]
        ]
        left = [a - alpha * b for a, b in zip(left, image)] + [
            -alpha * b for b in image[len(left) :]
        ]
        if step + 1 < ITERS:
            following = product(left, left)
            ratio = following / norm
            heading = [a + ratio * b for a, b in zip(left, heading)] + left[len(heading) :]
            norm = following

    for i in range(nx):
        warm = grid[WARM, depth + i, 0:ny, 0:nz]
        end = jnp.zeros_like(warm)
        for k in range(ITERS + 1):
            value = basis[k, depth + i, 0:ny, 0:nz]
            if k < ITERS:
                warm = warm + moved[k] * value
            end = end + left[k] * value
        warm_out[i] = warm
        left_out[i] = end

    for copy, dz in z_copies:
        pl.when(exists((0, 0, dz)))(copy.wait_send)
    for copy, (dx, dy) in raw + fwd:
        pl.when(exists((dx, dy, 0)))(copy.wait_send)


def body(counts, warm, source, category, table, flags):
    nx, ny, nz = warm.shape
    depth = ITERS + 1
    plane, line = counts[0] * counts[1], counts[2]
    if nx < depth or nx % 2 or ny % SUB or nz != LANES or table.shape[0] > LANES:
        raise ValueError("block shape")
    wide, tall, short, long = nx + 2 * depth, ny + 2 * SUB, ny + SUB, nz + LANES
    table = table[None]
    any_spec = pl.BlockSpec(memory_space=pl.ANY)
    vmem = pl.BlockSpec(memory_space=pltpu.VMEM)
    shape = jax.ShapeDtypeStruct(warm.shape, jnp.float32)
    f32 = jnp.float32
    return pl.pallas_call(
        functools.partial(kernel, counts),
        out_shape=(shape, shape),
        in_specs=[any_spec] * 5,
        out_specs=(vmem, vmem),
        scratch_shapes=[
            pltpu.VMEM((FIELDS + 1, wide, tall, long), f32),
            pltpu.VMEM((ITERS + 1, wide, short, long), f32),
            pltpu.VMEM((2, wide, short, long), f32),
            pltpu.VMEM((wide, tall, long), f32),
            pltpu.VMEM((wide, short, long), f32),
            pltpu.VMEM((wide, short, long), f32),
            pltpu.VMEM((SUB, LANES), f32),
            pltpu.VMEM(table.shape, f32),
            pltpu.VMEM((2, nx, ny, nz), jnp.int32),
            pltpu.VMEM((nx, ny, nz), f32),
            pltpu.VMEM((2, nx, SUB, nz), f32),
            pltpu.VMEM((2, nx, ny, nz), f32),
            pltpu.VMEM((4, 1, LANES), f32),
            pltpu.VMEM((2, plane, 1, LANES), f32),
            pltpu.VMEM((2, line, 1, LANES), f32),
            pltpu.VMEM((plane * line, 1, LANES), f32),
            pltpu.SemaphoreType.DMA((5,)),
            pltpu.SemaphoreType.DMA((8,)),
            pltpu.SemaphoreType.DMA((8,)),
            pltpu.SemaphoreType.DMA((8,)),
            pltpu.SemaphoreType.DMA((8,)),
            pltpu.SemaphoreType.DMA((8,)),
            pltpu.SemaphoreType.DMA((8,)),
            pltpu.SemaphoreType.DMA((2,)),
            pltpu.SemaphoreType.DMA((2,)),
            pltpu.SemaphoreType.DMA((4,)),
            pltpu.SemaphoreType.DMA((4,)),
        ],
        compiler_params=pltpu.CompilerParams(collective_id=0, has_side_effects=True),
    )(warm, source, category, table, flags)


def solution(mesh):
    counts = tuple(mesh.shape[a] for a in AXES)
    spec = P("gx", "gy", "gz")
    return jax.shard_map(
        functools.partial(body, counts),
        mesh=mesh,
        in_specs=(spec, spec, spec, P(), spec),
        out_specs=(spec, spec),
        check_vma=False,
    )
```

```python
import functools

import jax
import jax.numpy as jnp
from jax import lax
from jax.experimental import pallas as pl
from jax.experimental.pallas import tpu as pltpu
from jax.sharding import PartitionSpec as P

ITERS = 4
interval_delta = 2.0
cooling = 3.0

MESH = pl.DeviceIdType.MESH
AXES = ("gx", "gy", "gz")
SUB = 8
DIRECT = 64
LANES = 128
FIELDS = 4
WARM, COND, SOURCE, FLAGS, EDGES = range(5)
SLOT = LANES // FIELDS
PAIRS = [(i, j) for i in range(ITERS + 1) for j in range(i, ITERS + 1) if i < ITERS]


def smooth(values, axis):
    size = values.shape[axis]
    return (values + values) + (pltpu.roll(values, 1, axis) + pltpu.roll(values, size - 1, axis))


def smooth_all(before, center, after):
    return smooth(smooth(before + (center + center) + after, 0), 1)


def kernel(
    counts,
    warm_in,
    source_in,
    category_in,
    table_in,
    flags_in,
    both_out,
    grid,
    basis,
    flux,
    warm_flux,
    diag,
    couple,
    table,
    table_row,
    ints,
    edges,
    mixed,
    beside,
    row_out,
    plane_rows,
    line_rows,
    all_rows,
    load_sems,
    raw_send,
    raw_recv,
    mix_send,
    mix_recv,
    fwd_send,
    fwd_recv,
    z_send,
    z_recv,
    row_send,
    row_recv,
):
    plane, line = counts[0] * counts[1], counts[2]
    nx, ny, nz = both_out.shape[1:]
    depth = ITERS + 1
    wide, tall, long = grid.shape[1:]
    short = ny + SUB
    here = [lax.axis_index(a) for a in AXES]
    in_plane = here[0] * counts[1] + here[1]
    plane_targets = [
        {"gx": other // counts[1], "gy": other % counts[1], "gz": here[2]}
        for other in [(in_plane + step) % plane for step in range(1, plane)]
    ]
    line_targets = [
        {"gx": here[0], "gy": here[1], "gz": (here[2] + step) % line} for step in range(1, line)
    ]

    loads = [
        pltpu.make_async_copy(category_in, ints.at[0], load_sems.at[0]),
        pltpu.make_async_copy(flags_in, ints.at[1], load_sems.at[1]),
        pltpu.make_async_copy(
            warm_in, grid.at[WARM, pl.ds(depth, nx), pl.ds(0, ny), pl.ds(0, nz)], load_sems.at[2]
        ),
        pltpu.make_async_copy(
            source_in, grid.at[SOURCE, pl.ds(depth, nx), pl.ds(0, ny), pl.ds(0, nz)], load_sems.at[3]
        ),
        pltpu.make_async_copy(table_in, table_row, load_sems.at[4]),
    ]
    for load in loads:
        load.start()

    for f in range(FIELDS + 1):
        grid[f, 0:depth, :, 0:nz] = jnp.zeros((depth, tall, nz), jnp.float32)
        grid[f, depth + nx :, :, 0:nz] = jnp.zeros((depth, tall, nz), jnp.float32)
        grid[f, depth : depth + nx, ny:, 0:nz] = jnp.zeros((nx, tall - ny, nz), jnp.float32)
    beside[...] = jnp.zeros(beside.shape, jnp.float32)
    table[...] = jnp.zeros(table.shape, jnp.float32)
    moved_by = [[(here[k] + step) % counts[k] for step in range(counts[k])] for k in range(3)]
    all_targets = [
        {"gx": moved_by[0][a], "gy": moved_by[1][b], "gz": moved_by[2][c]}
        for c in reversed(range(counts[2]))
        for b in reversed(range(counts[1]))
        for a in reversed(range(counts[0]))
        if a or b or c
    ]

    barrier = pltpu.get_barrier_semaphore()

    for target in plane_targets + line_targets:
        pl.semaphore_signal(barrier, inc=1, device_id=target, device_id_type=MESH)

    for load in loads:
        load.wait()

    table[0:1, 0 : table_in.shape[1]] = table_row[...]
    lookup = jnp.broadcast_to(table[0:1, :], (ny, LANES))
    lane = lax.broadcasted_iota(jnp.int32, (ny, LANES), 1)
    top = jnp.zeros((ny, LANES), jnp.float32)
    total = jnp.zeros((ny, LANES), jnp.float32)
    most = jnp.zeros((ny, LANES), jnp.float32)
    least = jnp.ones((ny, LANES), jnp.float32)
    for i in range(nx):
        cond = jnp.take_along_axis(lookup, ints[0, i], axis=1)
        flag = ints[1, i].astype(jnp.float32)
        grid[COND, depth + i, 0:ny, 0:nz] = cond
        grid[FLAGS, depth + i, 0:ny, 0:nz] = flag
        pieces = [
            grid[WARM, depth + i, 0:ny, 0:nz],
            cond,
            grid[SOURCE, depth + i, 0:ny, 0:nz],
            flag,
        ]
        packed = None
        for f, piece in enumerate(pieces):
            turned = pltpu.roll(piece, (f * SLOT + SLOT // 2) % LANES, 1)
            packed = turned if packed is None else jnp.where(lane // SLOT == f, turned, packed)
        edges[i] = packed
        upper = lax.broadcasted_iota(jnp.int32, (SUB, nz), 0) < SUB // 2
        last, first = slice(ny - SUB, ny), slice(0, SUB)
        mixed[0, i] = jnp.where(
            upper, pltpu.roll(flag[last], SUB // 2, 0), grid[SOURCE, depth + i, last, 0:nz]
        )
        mixed[1, i] = jnp.where(
            upper, grid[SOURCE, depth + i, first, 0:nz], pltpu.roll(flag[first], SUB // 2, 0)
        )
        top = jnp.maximum(top, cond)
        total = total + cond
        most = jnp.maximum(most, flag)
        least = jnp.minimum(least, flag)
    shrink = lambda op, v: op(op(v, axis=0, keepdims=True), axis=1, keepdims=True)
    mean = shrink(jnp.sum, total) * (1.0 / (nx * ny * nz))
    high = 1.0 + interval_delta * cooling * shrink(jnp.max, most)
    high = high + 8.0 * interval_delta * (shrink(jnp.max, top) + mean)
    low = 1.0 + interval_delta * cooling * shrink(jnp.min, least)
    row_lane = lax.broadcasted_iota(jnp.int32, (1, LANES), 1)
    row = jnp.where(row_lane == 0, high, -low)
    row_out[0] = row
    plane_rows[0, in_plane] = row

    pl.semaphore_wait(barrier, plane + line - 2)

    def remote(src, dst, send, recv, offset):
        return pltpu.make_async_remote_copy(
            src_ref=src,
            dst_ref=dst,
            send_sem=send,
            recv_sem=recv,
            device_id={a: here[k] + offset[k] for k, a in enumerate(AXES)},
            device_id_type=MESH,
        )

    def exists(offset):
        good = None
        for k in range(3):
            if offset[k] > 0:
                one = here[k] < counts[k] - 1
            elif offset[k] < 0:
                one = here[k] > 0
            else:
                continue
            good = one if good is None else jnp.logical_and(good, one)
        return good

    def share(stage, rows_ref, slot, targets):
        for target in targets:
            pltpu.make_async_remote_copy(
                src_ref=row_out.at[stage],
                dst_ref=rows_ref.at[slot],
                send_sem=row_send.at[stage],
                recv_sem=row_recv.at[stage],
                device_id=target,
                device_id_type=MESH,
            ).start()

    def share_wait(stage, rows_ref, targets):
        if targets:
            whole = pltpu.make_async_remote_copy(
                src_ref=rows_ref.at[pl.ds(0, len(targets))],
                dst_ref=rows_ref.at[pl.ds(0, len(targets))],
                send_sem=row_send.at[stage],
                recv_sem=row_recv.at[stage],
                device_id=targets[0],
                device_id_type=MESH,
            )
            whole.wait_send()
            whole.wait_recv()

    share(0, plane_rows.at[0], in_plane, plane_targets)

    z_copies = []
    for k, dz in enumerate((1, -1)):
        copy = remote(edges, beside.at[k], z_send.at[k], z_recv.at[k], (0, 0, dz))
        z_copies.append((copy, dz))
        pl.when(exists((0, 0, dz)))(copy.start)

    def ranges(offset):
        dx, dy = offset
        if dx == 0:
            xs, xd, xn = depth, depth, nx
        elif dx > 0:
            xs, xd, xn = nx, 0, depth
        else:
            xs, xd, xn = depth, depth + nx, depth
        if dy == 0:
            ys, yd, yn = 0, 0, ny
        elif dy > 0:
            ys, yd, yn = ny - SUB, ny + SUB, SUB
        else:
            ys, yd, yn = 0, ny, SUB
        z = pl.ds(0, nz)
        return (pl.ds(xs, xn), pl.ds(ys, yn), z), (pl.ds(xd, xn), pl.ds(yd, yn), z)

    offsets = [(0, 1), (0, -1), (1, 1), (-1, -1), (1, -1), (-1, 1), (1, 0), (-1, 0)]

    raw, fwd = [], []
    for k, offset in enumerate(offsets):
        src, dst = ranges(offset)
        full = offset + (0,)
        count = FIELDS if offset[1] == 0 else SOURCE
        fields = (pl.ds(0, count),)
        raw.append(
            (
                remote(
                    grid.at[fields + src], grid.at[fields + dst], raw_send.at[k], raw_recv.at[k], full
                ),
                offset,
            )
        )
        if offset[1] != 0:
            xs = pl.ds(src[0].start - depth, src[0].size)
            raw.append(
                (
                    remote(
                        mixed.at[0 if offset[1] > 0 else 1, xs],
                        grid.at[(SOURCE,) + dst],
                        mix_send.at[k],
                        mix_recv.at[k],
                        full,
                    ),
                    offset,
                )
            )
        fwd.append(
            (
                remote(
                    grid.at[(EDGES,) + src], grid.at[(EDGES,) + dst], fwd_send.at[k], fwd_recv.at[k], full
                ),
                offset,
            )
        )
    for copy, (dx, dy) in raw:
        pl.when(exists((dx, dy, 0)))(copy.start)

    for copy, dz in z_copies:
        pl.when(exists((0, 0, -dz)))(copy.wait_recv)
    low_half = lane % SLOT < SLOT // 2
    for i in range(nx):
        grid[EDGES, depth + i, 0:ny, 0:nz] = jnp.where(low_half, beside[0, i], beside[1, i])
    for copy, (dx, dy) in fwd:
        pl.when(exists((dx, dy, 0)))(copy.start)

    share_wait(0, plane_rows.at[0], plane_targets)
    row = jnp.max(plane_rows[0], axis=0)
    row_out[1] = row
    line_rows[0, here[2]] = row
    share(1, line_rows.at[0], here[2], line_targets)

    for copy, (dx, dy) in raw:
        pl.when(exists((-dx, -dy, 0)))(copy.wait_recv)
    for copy, (dx, dy) in fwd:
        pl.when(exists((-dx, -dy, 0)))(copy.wait_recv)

    batch = next(u for u in (6, 4, 2) if wide % u == 0)

    @pl.loop(0, wide // batch)
    def _(group):
        for u in range(batch):
            i = batch * group + u
            packed = grid[EDGES, i, :, 0:nz]
            grid[FLAGS, i, ny:, 0:nz] = jnp.concatenate(
                [
                    pltpu.roll(grid[SOURCE, i, ny : ny + SUB, 0:nz], SUB // 2, 0),
                    pltpu.roll(grid[SOURCE, i, ny + SUB :, 0:nz], SUB // 2, 0),
                ],
                axis=0,
            )
            for f in range(FIELDS):
                grid[f, i, :, nz:] = pltpu.roll(packed, (-f * SLOT - SLOT // 2) % LANES, 1)
            warm_flux[i] = grid[COND, i] * grid[WARM, i]

    share_wait(1, line_rows.at[0], line_targets)
    bounds = jnp.max(line_rows[0], axis=0)
    pick = lambda v, i: jnp.sum(jnp.where(row_lane == i, v, 0.0), axis=1, keepdims=True)
    high, low = pick(bounds, 0), -pick(bounds, 1)
    middle = 0.5 * (high + low)
    half = 0.5 * (high - low)
    twice = 2.0 / half

    def valid(index, size, cut, k):
        inner = index < size
        right = jnp.logical_and(index < size + cut, here[k] < counts[k] - 1)
        left = jnp.logical_and(index >= size + cut, here[k] > 0)
        return jnp.logical_or(inner, jnp.logical_or(right, left))

    def inside_of(rows, cut):
        y_index = lax.broadcasted_iota(jnp.int32, (rows, long), 0)
        z_index = lax.broadcasted_iota(jnp.int32, (rows, long), 1)
        both = jnp.logical_and(valid(y_index, ny, cut, 1), valid(z_index, nz, LANES // 2, 2))
        return jnp.where(both, 1.0, 0.0)

    x_left = jnp.where(here[0] > 0, 1.0, 0.0)
    x_right = jnp.where(here[0] < counts[0] - 1, 1.0, 0.0)

    def x_inside(i):
        return jnp.where(i < depth, x_left, jnp.where(i >= depth + nx, x_right, 1.0))

    quarter = 0.125 * interval_delta
    inside = quarter * inside_of(tall, SUB)
    first_half = lax.broadcasted_iota(jnp.int32, (SUB, long), 0) < SUB // 2

    def narrow(v):
        ends = jnp.where(first_half, v[ny : ny + SUB], v[ny + SUB :])
        return jnp.concatenate([v[:ny], ends], axis=0)

    several = next(u for u in (4, 2) if (wide - 2) % u == 0)

    @pl.loop(0, (wide - 2) // several)
    def _(group):
        for u in range(several):
            i = 1 + several * group + u
            cond = grid[COND, i]
            ring = smooth_all(grid[COND, i - 1], cond, grid[COND, i + 1])
            d = 1.0 + interval_delta * cooling * grid[FLAGS, i]
            d = d + 8.0 * interval_delta * cond + quarter * ring
            warm = grid[WARM, i]
            own = smooth_all(grid[WARM, i - 1], warm, grid[WARM, i + 1])
            push = smooth_all(warm_flux[i - 1], warm_flux[i], warm_flux[i + 1])
            image = d * warm - (quarter * cond * own + x_inside(i) * inside * push)
            left = narrow(warm + interval_delta * grid[SOURCE, i] - image)
            edge = (quarter * twice) * narrow(cond)
            basis[0, i] = left
            diag[i] = twice * (narrow(d) - middle)
            couple[i] = edge
            flux[0, i] = edge * left

    within = inside_of(short, SUB // 2)
    for k in range(ITERS):

        half_planes = wide // 2 - 2 - k

        @pl.loop(0, 2)
        def _(group):
            for u in range(half_planes):
                i = 2 + k + half_planes * group + u
                edge = couple[i]
                mid = basis[k, i]
                own = smooth_all(basis[k, i - 1], mid, basis[k, i + 1])
                push = smooth_all(flux[k % 2, i - 1], flux[k % 2, i], flux[k % 2, i + 1])
                fresh = diag[i] * mid - (edge * own + x_inside(i) * within * push)
                if k > 0:
                    fresh = fresh - basis[k - 1, i]
                basis[k + 1, i] = fresh
                if k + 1 < ITERS:
                    flux[(k + 1) % 2, i] = edge * fresh

    sums = [None] * len(PAIRS)
    for i in range(depth, depth + nx):
        rows = [basis[k, i, 0:ny, 0:nz] for k in range(ITERS + 1)]
        for n, (a, b) in enumerate(PAIRS):
            term = rows[a] * rows[b]
            sums[n] = term if sums[n] is None else sums[n] + term
    diagonal = lax.broadcasted_iota(jnp.int32, (SUB, LANES), 0)
    across = lax.broadcasted_iota(jnp.int32, (SUB, LANES), 1)
    row = jnp.zeros((SUB, LANES), jnp.float32)
    for start in range(0, len(PAIRS), SUB):
        tile = jnp.zeros((SUB, LANES), jnp.float32)
        for n in range(start, min(start + SUB, len(PAIRS))):
            tile = jnp.where(diagonal == n - start, jnp.sum(sums[n], axis=0, keepdims=True), tile)
        column = jnp.sum(tile, axis=1, keepdims=True)
        row = row + jnp.where(across == diagonal + start, column, 0.0)
    row = jnp.sum(row, axis=0, keepdims=True)
    row_out[2] = row
    if plane * line <= DIRECT:
        mine = in_plane * line + here[2]
        all_rows[mine] = row
        share(2, all_rows, mine, all_targets)
        share_wait(2, all_rows, all_targets)
        row = jnp.sum(all_rows[...], axis=0)
    else:
        plane_rows[1, in_plane] = row
        share(2, plane_rows.at[1], in_plane, plane_targets)
        share_wait(2, plane_rows.at[1], plane_targets)
        row = jnp.sum(plane_rows[1], axis=0)
        row_out[3] = row
        line_rows[1, here[2]] = row
        share(3, line_rows.at[1], here[2], line_targets)
        share_wait(3, line_rows.at[1], line_targets)
        row = jnp.sum(line_rows[1], axis=0)
    gram = {}
    for n, (a, b) in enumerate(PAIRS):
        gram[a, b] = gram[b, a] = pick(row, n)

    def apply(p):
        q = [middle * a for a in p] + [jnp.zeros_like(half)]
        for i, a in enumerate(p):
            q[i + 1] = q[i + 1] + (0.5 * half) * a
            if i > 0:
                q[i - 1] = q[i - 1] + (0.5 * half) * a
        return q

    def product(p, q):
        value = None
        for i, a in enumerate(p):
            inner = None
            for j, b in enumerate(q):
                term = gram[i, j] * b
                inner = term if inner is None else inner + term
            inner = a * inner
            value = inner if value is None else value + inner
        return value

    left = [jnp.ones_like(half)]
    heading = list(left)
    moved = []
    norm = product(left, left)
    for step in range(ITERS):
        image = apply(heading)
        alpha = norm / product(heading, image)
        moved = [a + alpha * b for a, b in zip(moved, heading)] + [
            alpha * b for b in heading[len(moved) :]
        ]
        left = [a - alpha * b for a, b in zip(left, image)] + [
            -alpha * b for b in image[len(left) :]
        ]
        if step + 1 < ITERS:
            following = product(left, left)
            ratio = following / norm
            heading = [a + ratio * b for a, b in zip(left, heading)] + left[len(heading) :]
            norm = following

    for i in range(nx):
        warm = grid[WARM, depth + i, 0:ny, 0:nz]
        end = jnp.zeros_like(warm)
        for k in range(ITERS + 1):
            value = basis[k, depth + i, 0:ny, 0:nz]
            if k < ITERS:
                warm = warm + moved[k] * value
            end = end + left[k] * value
        both_out[0, i] = warm
        both_out[1, i] = end

    for copy, dz in z_copies:
        pl.when(exists((0, 0, dz)))(copy.wait_send)
    for copy, (dx, dy) in raw + fwd:
        pl.when(exists((dx, dy, 0)))(copy.wait_send)


def body(counts, warm, source, category, table, flags):
    nx, ny, nz = warm.shape
    depth = ITERS + 1
    plane, line = counts[0] * counts[1], counts[2]
    if nx < depth or nx % 2 or ny % SUB or nz != LANES or table.shape[0] > LANES:
        raise ValueError("block shape")
    wide, tall, short, long = nx + 2 * depth, ny + 2 * SUB, ny + SUB, nz + LANES
    table = table[None]
    any_spec = pl.BlockSpec(memory_space=pl.ANY)
    vmem = pl.BlockSpec(memory_space=pltpu.VMEM)
    f32 = jnp.float32
    both = pl.pallas_call(
        functools.partial(kernel, counts),
        out_shape=pltpu.VMEM((2,) + warm.shape, jnp.float32),
        in_specs=[any_spec] * 5,
        out_specs=vmem,
        scratch_shapes=[
            pltpu.VMEM((FIELDS + 1, wide, tall, long), f32),
            pltpu.VMEM((ITERS + 1, wide, short, long), f32),
            pltpu.VMEM((2, wide, short, long), f32),
            pltpu.VMEM((wide, tall, long), f32),
            pltpu.VMEM((wide, short, long), f32),
            pltpu.VMEM((wide, short, long), f32),
            pltpu.VMEM((SUB, LANES), f32),
            pltpu.VMEM(table.shape, f32),
            pltpu.VMEM((2, nx, ny, nz), jnp.int32),
            pltpu.VMEM((nx, ny, nz), f32),
            pltpu.VMEM((2, nx, SUB, nz), f32),
            pltpu.VMEM((2, nx, ny, nz), f32),
            pltpu.VMEM((4, 1, LANES), f32),
            pltpu.VMEM((2, plane, 1, LANES), f32),
            pltpu.VMEM((2, line, 1, LANES), f32),
            pltpu.VMEM((plane * line, 1, LANES), f32),
            pltpu.SemaphoreType.DMA((5,)),
            pltpu.SemaphoreType.DMA((8,)),
            pltpu.SemaphoreType.DMA((8,)),
            pltpu.SemaphoreType.DMA((8,)),
            pltpu.SemaphoreType.DMA((8,)),
            pltpu.SemaphoreType.DMA((8,)),
            pltpu.SemaphoreType.DMA((8,)),
            pltpu.SemaphoreType.DMA((2,)),
            pltpu.SemaphoreType.DMA((2,)),
            pltpu.SemaphoreType.DMA((4,)),
            pltpu.SemaphoreType.DMA((4,)),
        ],
        compiler_params=pltpu.CompilerParams(collective_id=0, has_side_effects=True),
    )(warm, source, category, table, flags)
    return both[0], both[1]


def solution(mesh):
    counts = tuple(mesh.shape[a] for a in AXES)
    spec = P("gx", "gy", "gz")
    return jax.shard_map(
        functools.partial(body, counts),
        mesh=mesh,
        in_specs=(spec, spec, spec, P(), spec),
        out_specs=(spec, spec),
        check_vma=False,
    )
```
